32 devices in a mesh: shots: 2 (over y), rx: 4 (over z), ta: 2 (over x), af: 2 (over core).
Axes of the slice: x: 2, y: 2, z: 4, core: 2. Of those that a mesh axis runs over, the one named last changes fastest.
Arguments:
- traces: bfloat16 [4096, 512], P(('shots', 'rx'), ('ta', 'af')), parts along dimension 0, may hold values from -6 to 6
- slopes: int32 [512], replicated, may hold values from 0 to 1023
- offsets: int32 [4096], P('shots'), parts along dimension 0, may hold values from 1 to 4095
- live: int32 [4096], P('shots'), parts along dimension 0, may hold values 0 or 1
Outputs:
- stack: float32 [1024, 512], P(('shots', 'rx'), ('ta', 'af')), parts along dimension 0
- coherence: float32 [1024, 512], P(('shots', 'rx'), ('ta', 'af')), parts along dimension 0
- peak_values: float32 [1024], P(('shots', 'rx')), parts along dimension 0
The draws below stay inside these ranges and needn't reach their ends.
There are 2 independent parts, one for each index of `shots`. The reference program is written for one: setup_inputs(seed, part) draws one part's arguments, and reference() takes and returns one part's arrays. A program takes and returns all parts, laid end to end along the dimension named above; an argument that names none is the same for every part. Nothing has to cross between parts.
Inputs may be any that keep to these rules, and one draw needn't show every extreme that they name: delays are below 64: (slopes * offsets) // 65536 < 64.
All inputs are finite; a program needn't handle non-finite values.
Results may differ from the reference program's by a relative error of at most 0.0003.
Values may be sent and summed in bfloat16 or wider, within the bound.
No kernel may reach another device: no remote copies, remote signals or barrier semaphores. Data moves between devices by JAX's collectives and lax.ppermute only.
A program may use at most 64 MiB of HBM per device.

```python
import jax
import jax.numpy as jnp
from jax import lax

RECV = 2048
SLOWS = 512
SPAN = 64
WIN = 16
NT = 512


def with_ends(values, rng, smallest, largest):
    index_at = [jax.random.randint(jax.random.fold_in(rng, axis), (), 0, length) for axis, length in enumerate(values.shape)]
    widest = values.shape.index(max(values.shape))
    neighbour = index_at[:widest] + [(index_at[widest] + 1) % values.shape[widest]] + index_at[widest + 1:]
    return values.at[tuple(index_at)].set(smallest).at[tuple(neighbour)].set(largest)


def steps_of(key, extent, cuts, smallest, high):
    factor_of = 1.0
    for position, shards_of in cuts:
        heights = jax.random.uniform(jax.random.fold_in(jax.random.fold_in(key, 6), position), (shards_of,), jnp.float32, smallest / len(cuts), high / len(cuts))
        factor_of = factor_of * jnp.repeat(jnp.exp(heights), extent[position] // shards_of).reshape((-1,) + (1,) * (len(extent) - 1 - position))
    return factor_of


def gaussian(key, extent, scale, limit, shards=(), held_as=jnp.bfloat16):
    result = scale * jax.random.normal(key, extent, jnp.float32)
    if shards:
        result = result * steps_of(key, extent, shards, -0.22, 0.18)
    return jnp.clip(result, -limit, limit).astype(held_as)


def setup_inputs(seed: int = 0, part: int = 0) -> dict:
    key_of = jax.random.split(jax.random.key(seed), 5)
    part_splits = jax.random.split(jax.random.fold_in(key_of[4], part), 5)
    traces = gaussian(part_splits[0], (RECV, NT), 1.0, 6.0, ((0, 4), (1, 4)))
    slopes = with_ends(jax.random.randint(key_of[1], (SLOWS,), 0, 16 * SPAN), jax.random.fold_in(key_of[1], 1), 0, (16 * SPAN) - 1).astype(jnp.int32)
    offsets = with_ends(jax.random.randint(part_splits[2], (RECV,), 1, 4096), jax.random.fold_in(part_splits[2], 1), 1, 4095).astype(jnp.int32)
    live = with_ends((jax.random.randint(part_splits[3], (RECV,), 0, 8) < 7).astype(jnp.int32), jax.random.fold_in(part_splits[3], 1), 0, 1)
    return dict(traces=traces, slopes=slopes, offsets=offsets, live=live)


def reference(traces, slopes, offsets, live):
    delays = (slopes[:, None] * offsets[None, :]) // 65536
    weighted = traces * live.astype(jnp.bfloat16)[:, None]
    squares = (weighted.astype(jnp.float32) ** 2).astype(jnp.bfloat16)
    padded_x = jnp.pad(weighted, ((0, 0), (0, SPAN)))
    padded_s = jnp.pad(squares, ((0, 0), (0, SPAN)))

    def lag_step(lag_index, carry):
        stack_acc, energy_acc = carry
        onehot = (delays == lag_index).astype(jnp.bfloat16)
        part_x = lax.dynamic_slice_in_dim(padded_x, lag_index, NT, 1)
        part_s = lax.dynamic_slice_in_dim(padded_s, lag_index, NT, 1)
        stack_acc = stack_acc + jnp.dot(onehot, part_x, preferred_element_type=jnp.float32)
        energy_acc = energy_acc + jnp.dot(onehot, part_s, preferred_element_type=jnp.float32)
        return stack_acc, energy_acc

    zeros = jnp.zeros((SLOWS, NT), jnp.float32)
    stack, energy = lax.fori_loop(0, SPAN, lag_step, (zeros, zeros))
    long_stack = jnp.pad(stack, ((0, 0), (0, WIN)))
    long_energy = jnp.pad(energy, ((0, 0), (0, WIN)))
    power_sum = jnp.zeros((SLOWS, NT), jnp.float32)
    energy_sum = jnp.zeros((SLOWS, NT), jnp.float32)
    for lag_index in range(WIN):
        power_sum = power_sum + long_stack[:, lag_index:lag_index + NT] ** 2
        energy_sum = energy_sum + long_energy[:, lag_index:lag_index + NT]
    coherence = power_sum / jnp.maximum(energy_sum, 1.0)
    peak_values = jnp.max(coherence, axis=1)
    return stack, coherence, peak_values
```

```python
import functools

import jax
import jax.numpy as jnp
from jax import lax
from jax.experimental import pallas as pl
from jax.experimental.pallas import tpu as pltpu
from jax.sharding import PartitionSpec as P

SPAN = 64
WIN = 16
GROUP = 4
PACK = 16


def passed_along(value, axis, steps):
    count = lax.axis_size(axis)
    leading, last = (max(0, -steps), min(count, count - steps))
    return lax.ppermute(value, axis, [(source, source + steps) for source in range(leading, last)])


def stack_kernel(traces, halo, gain, offsets, slopes, out, samples, shifted, delays, acc, *, cols, row_blk, col_blk):
    rows, block_len = traces.shape
    rest = halo.shape[1]
    slows = slopes.shape[1]
    weighted = jnp.concatenate(
        [traces[...].astype(jnp.float32), halo[...].astype(jnp.float32)], axis=1
    ) * gain[...].astype(jnp.float32)
    turned = weighted.T
    filled = block_len + rest
    samples[0, 0:filled, :] = turned
    samples[1, 0:filled, :] = (turned * turned).astype(jnp.bfloat16).astype(jnp.float32)
    delays[...] = ((offsets[...] * slopes[...]) >> 16).astype(jnp.float32).astype(jnp.bfloat16)
    reach = shifted.shape[2]
    for phase in range(PACK):
        shifted[phase] = samples[:, phase : phase + reach, :].astype(jnp.bfloat16)
    acc[...] = jnp.zeros_like(acc)
    for row in range(0, rows, row_blk):
        for col in range(0, slows, col_blk):

            def body(step, carry, row=row, col=col):
                first = step * GROUP
                left, right = [], []
                here = delays[row : row + row_blk, col : col + col_blk]
                for lag in range(GROUP):
                    at = first + lag
                    start = pl.multiple_of((at // PACK) * PACK, PACK)
                    part = [
                        shifted[at % PACK, half, pl.ds(start, cols), row : row + row_blk] for half in range(2)
                    ]
                    left.append(jnp.concatenate(part, axis=0))
                    hit = here == at.astype(jnp.float32).astype(jnp.bfloat16)
                    right.append(jnp.where(hit, jnp.bfloat16(1), jnp.bfloat16(0)))
                acc[:, col : col + col_blk] += jnp.dot(
                    jnp.concatenate(left, axis=1),
                    jnp.concatenate(right, axis=0),
                    preferred_element_type=jnp.float32,
                )
                return carry

            lax.fori_loop(0, SPAN // GROUP, body, 0)
    groups, _, width = out.shape
    for group in range(groups):
        out[group] = acc[:, group * width : (group + 1) * width]


def semblance_kernel(parts, stack, coherence, peak, sums, *, cols, block_len):
    total = parts[0]
    for group in range(1, parts.shape[0]):
        total = total + parts[group]
    power = total[:cols] * total[:cols]
    energy = total[cols:]
    stack[...] = total[:block_len].T
    sums[0] = power
    sums[1] = energy
    length, reach = cols, 1
    while reach < WIN:
        length = length - reach
        sums[:, 0:length] = sums[:, 0:length] + sums[:, reach : reach + length]
        reach *= 2
    result = sums[0, 0:block_len] / jnp.maximum(sums[1, 0:block_len], 1.0)
    coherence[...] = result.T
    peak[...] = jnp.max(result, axis=0, keepdims=True)


def largest(value, axes):
    for axis in axes[::-1]:
        count = lax.axis_size(axis)
        step = 1
        if count & (count - 1):
            value = lax.pmax(value, axis)
            continue
        while step < count:
            other = lax.ppermute(value, axis, [(i, i ^ step) for i in range(count)])
            value = jnp.maximum(value, other)
            step *= 2
    return value


def on_device(traces, slopes, offsets, live):
    receiver_group = lax.axis_index("rx")
    groups = lax.axis_size("rx")
    rows, block_len = traces.shape
    slows = slopes.shape[0]
    width = slows // groups
    rest = SPAN + WIN
    cols = block_len + WIN
    halo = passed_along(traces[:, :rest], ("ta", "af"), -1)
    gain = lax.dynamic_slice_in_dim(live, receiver_group * rows, rows)
    offset_local = lax.dynamic_slice_in_dim(offsets, receiver_group * rows, rows)
    row_blk, col_blk = min(256, rows), min(256, slows)
    partial = pl.pallas_call(
        functools.partial(stack_kernel, cols=cols, row_blk=row_blk, col_blk=col_blk),
        out_shape=jax.ShapeDtypeStruct((groups, 2 * cols, width), jnp.float32),
        scratch_shapes=[
            pltpu.VMEM((2, block_len + rest, rows), jnp.float32),
            pltpu.VMEM((PACK, 2, block_len + rest - PACK, rows), jnp.bfloat16),
            pltpu.VMEM((rows, slows), jnp.bfloat16),
            pltpu.VMEM((2 * cols, slows), jnp.float32),
        ],
        name="stack",
    )(traces, halo, gain[:, None], offset_local[:, None], slopes[None, :])
    parts = lax.all_to_all(partial, "rx", split_axis=0, concat_axis=0, tiled=True)
    stack, coherence, peak = pl.pallas_call(
        functools.partial(semblance_kernel, cols=cols, block_len=block_len),
        out_shape=(
            jax.ShapeDtypeStruct((width, block_len), jnp.float32),
            jax.ShapeDtypeStruct((width, block_len), jnp.float32),
            jax.ShapeDtypeStruct((1, width), jnp.float32),
        ),
        scratch_shapes=[pltpu.VMEM((2, cols, width), jnp.float32)],
        name="semblance",
    )(parts)
    return (stack, coherence, largest(peak, ("ta", "af")).reshape(width))


def solution(mesh):
    placed = (P(("shots", "rx"), ("ta", "af")), P(), P("shots"), P("shots"))
    return jax.shard_map(
        on_device,
        mesh=mesh,
        in_specs=placed,
        out_specs=(
            P(("shots", "rx"), ("ta", "af")),
            P(("shots", "rx"), ("ta", "af")),
            P(("shots", "rx")),
        ),
        check_vma=False,
    )
```

```python
import functools

import jax
import jax.numpy as jnp
from jax import lax
from jax.experimental import pallas as pl
from jax.experimental.pallas import tpu as pltpu
from jax.sharding import PartitionSpec as P

SPAN = 64
WIN = 16
PACK = 16
LANES = 256


def passed_along(value, axis, steps):
    count = lax.axis_size(axis)
    leading, last = (max(0, -steps), min(count, count - steps))
    return lax.ppermute(value, axis, [(source, source + steps) for source in range(leading, last)])


def turned_about(value, axis, steps):
    count = lax.axis_size(axis)
    return lax.ppermute(value, axis, [(i, (i + steps) % count) for i in range(count)])


def stack_kernel(*refs, away, groups, cols, block_len, first, final):
    count = len(away)
    place, slopes, gain, offsets = refs[:4]
    traces = refs[4 : 4 + count]
    halos = refs[4 + count : 4 + 2 * count]
    refs = refs[4 + 2 * count :]
    if not first:
        before, refs = refs[0], refs[1:]
    if final:
        stack, coherence, peak = refs[:3]
        refs = refs[3:]
    else:
        out, refs = refs[0], refs[1:]
    total, left, right_hits, product = refs
    rows = traces[0].shape[0]
    tall = cols + PACK
    width = total.shape[1]
    reps = LANES // width
    me = place[0]
    slope_row = slopes[me].astype(jnp.float32)
    lag_row = lax.broadcasted_iota(jnp.int32, (1, LANES), 1) // width
    steps = SPAN // PACK
    if first:
        total[...] = jnp.zeros_like(total)
    else:
        total[...] = before[...]
    for index, distance in enumerate(away):
        group = lax.rem(me + (groups - distance), groups)
        live = gain[group].astype(jnp.float32)
        weighted = jnp.concatenate(
            [traces[index][...].astype(jnp.float32).T, halos[index][...].astype(jnp.float32).T], axis=0
        ) * live
        squares = weighted * weighted
        for step in range(steps):
            at = step * PACK
            here = slice(step * rows, (step + 1) * rows)
            left[0:tall, here] = weighted[at : at + tall].astype(jnp.bfloat16)
            left[tall:, here] = squares[at : at + tall].astype(jnp.bfloat16)
        offset_col = jnp.broadcast_to(offsets[group].astype(jnp.float32), (128, rows)).T[:, 0:1]
        delays = (offset_col * slope_row).astype(jnp.int32) >> 16
        right_hits[...] = (delays - lag_row).astype(jnp.float32).astype(jnp.bfloat16)
        for base in range(0, PACK, reps):
            hits = [
                jnp.where(right_hits[...] == jnp.bfloat16(step * PACK + base), jnp.bfloat16(1), jnp.bfloat16(0))
                for step in range(steps)
            ]
            product[...] = jnp.dot(
                left[...], jnp.concatenate(hits, axis=0), preferred_element_type=jnp.float32
            )
            for rep in range(reps):
                lanes = slice(rep * width, (rep + 1) * width)
                down = base + rep
                total[0:cols] += product[down : down + cols, lanes]
                total[cols:] += product[tall + down : tall + down + cols, lanes]
    if not final:
        out[...] = total[...]
        return
    result = total[...]
    stack[...] = result[:block_len].T
    total[0:cols] = result[:cols] * result[:cols]
    length, reach = cols, 1
    while reach < WIN:
        length = length - reach
        for start in (0, cols):
            total[start : start + length] = (
                total[start : start + length] + total[start + reach : start + reach + length]
            )
        reach *= 2
    ratio = total[0:block_len] / jnp.maximum(total[cols : cols + block_len], 1.0)
    coherence[...] = ratio.T
    peak[...] = jnp.max(ratio, axis=0, keepdims=True)


def largest(value, axes):
    for axis in axes[::-1]:
        count = lax.axis_size(axis)
        step = 1
        if count & (count - 1):
            value = lax.pmax(value, axis)
            continue
        while step < count:
            other = lax.ppermute(value, axis, [(i, i ^ step) for i in range(count)])
            value = jnp.maximum(value, other)
            step *= 2
    return value


def on_device(traces, slopes, offsets, live):
    groups = lax.axis_size("rx")
    rows, block_len = traces.shape
    width = slopes.shape[0] // groups
    rest = SPAN + WIN
    cols = block_len + WIN
    place = lax.axis_index("rx").astype(jnp.int32).reshape(1)
    halo = passed_along(traces[:, :rest], ("ta", "af"), -1)
    order = [0] + [d for pair in zip(range(1, groups), range(groups - 1, 0, -1)) for d in pair][: groups - 1]
    order = list(dict.fromkeys(order))
    moved = {d: traces if d == 0 else turned_about(traces, "rx", d) for d in order}
    beside = {d: halo if d == 0 else turned_about(halo, "rx", d) for d in order}
    calls = [part for part in (order[:1], order[1:3], order[3:]) if part]
    slope_rows = jnp.tile(slopes.reshape(groups, 1, width), (1, 1, LANES // width))
    gain = live.reshape(groups, 1, rows)
    offset_rows = offsets.reshape(groups, 1, rows)
    partial = []
    for number, part in enumerate(calls):
        final = number == len(calls) - 1
        share = jax.ShapeDtypeStruct((2 * cols, width), jnp.float32)
        panel = jax.ShapeDtypeStruct((width, block_len), jnp.float32)
        crest = jax.ShapeDtypeStruct((1, width), jnp.float32)
        tall = 2 * (cols + PACK)
        vmem = pl.BlockSpec(memory_space=pltpu.VMEM)
        result = pl.pallas_call(
            functools.partial(
                stack_kernel,
                away=part,
                groups=groups,
                cols=cols,
                block_len=block_len,
                first=number == 0,
                final=final,
            ),
            in_specs=[pl.BlockSpec(memory_space=pltpu.SMEM)] + [vmem] * (3 + 2 * len(part) + len(partial)),
            out_shape=(panel, panel, crest) if final else share,
            scratch_shapes=[
                pltpu.VMEM((2 * cols, width), jnp.float32),
                pltpu.VMEM((tall, rows * (SPAN // PACK)), jnp.bfloat16),
                pltpu.VMEM((rows, LANES), jnp.bfloat16),
                pltpu.VMEM((tall, LANES), jnp.float32),
            ],
            name=f"stack{number}",
        )(
            place,
            slope_rows,
            gain,
            offset_rows,
            *[moved[d] for d in part],
            *[beside[d] for d in part],
            *partial,
        )
        partial = [result]
    stack, coherence, peak = result
    return (stack, coherence, largest(peak, ("ta", "af")).reshape(width))


def solution(mesh):
    placed = (P(("shots", "rx"), ("ta", "af")), P(), P("shots"), P("shots"))
    return jax.shard_map(
        on_device,
        mesh=mesh,
        in_specs=placed,
        out_specs=(
            P(("shots", "rx"), ("ta", "af")),
            P(("shots", "rx"), ("ta", "af")),
            P(("shots", "rx")),
        ),
        check_vma=False,
    )
```

```python
import functools

import jax
import jax.numpy as jnp
from jax import lax
from jax.experimental import pallas as pl
from jax.experimental.pallas import tpu as pltpu
from jax.sharding import PartitionSpec as P

SPAN = 64
WIN = 16
PACK = 16
LANES = 256


def passed_along(value, axis, steps):
    count = lax.axis_size(axis)
    leading, last = (max(0, -steps), min(count, count - steps))
    return lax.ppermute(value, axis, [(source, source + steps) for source in range(leading, last)])


def turned_about(value, axis, steps):
    count = lax.axis_size(axis)
    return lax.ppermute(value, axis, [(i, (i + steps) % count) for i in range(count)])


def near(value):
    return pltpu.with_memory_space_constraint(value, pltpu.VMEM)


def stack_kernel(*refs, away, groups, cols, block_len, first, final):
    count = len(away)
    place, slopes, gain, offsets = refs[:4]
    traces = refs[4 : 4 + count]
    refs = refs[4 + count :]
    if not first:
        before, refs = refs[0], refs[1:]
    if final:
        stack, coherence, peak = refs[:3]
        refs = refs[3:]
    else:
        out, refs = refs[0], refs[1:]
    total, left, right_hits, product = refs
    rows = traces[0].shape[0]
    tall = cols + PACK
    width = total.shape[1]
    reps = LANES // width
    me = place[0]
    slope_row = slopes[me].astype(jnp.float32)
    if slope_row.shape[1] < LANES:
        slope_row = jnp.concatenate([slope_row] * reps, axis=1)
    lag_row = lax.broadcasted_iota(jnp.int32, (1, LANES), 1) // width
    steps = SPAN // PACK
    if first:
        total[...] = jnp.zeros_like(total)
    else:
        total[...] = before[...]
    for index, distance in enumerate(away):
        group = lax.rem(me + (groups - distance), groups)
        live = gain[group].astype(jnp.float32)
        weighted = traces[index][...].astype(jnp.float32).T * live
        squares = weighted * weighted
        for step in range(steps):
            at = step * PACK
            here = slice(step * rows, (step + 1) * rows)
            left[0:tall, here] = weighted[at : at + tall].astype(jnp.bfloat16)
            left[tall:, here] = squares[at : at + tall].astype(jnp.bfloat16)
        offset_col = jnp.broadcast_to(offsets[group].astype(jnp.float32), (128, rows)).T[:, 0:1]
        delays = (offset_col * slope_row).astype(jnp.int32) >> 16
        right_hits[...] = (delays - lag_row).astype(jnp.float32).astype(jnp.bfloat16)
        for base in range(0, PACK, reps):
            hits = [
                jnp.where(right_hits[...] == jnp.bfloat16(step * PACK + base), jnp.bfloat16(1), jnp.bfloat16(0))
                for step in range(steps)
            ]
            product[...] = jnp.dot(
                left[...], jnp.concatenate(hits, axis=0), preferred_element_type=jnp.float32
            )
            for rep in range(reps):
                lanes = slice(rep * width, (rep + 1) * width)
                down = base + rep
                total[0:cols] += product[down : down + cols, lanes]
                total[cols:] += product[tall + down : tall + down + cols, lanes]
    if not final:
        out[...] = total[...]
        return
    result = total[...]
    stack[...] = result[:block_len].T
    total[0:cols] = result[:cols] * result[:cols]
    length, reach = cols, 1
    while reach < WIN:
        length = length - reach
        for start in (0, cols):
            total[start : start + length] = (
                total[start : start + length] + total[start + reach : start + reach + length]
            )
        reach *= 2
    ratio = total[0:block_len] / jnp.maximum(total[cols : cols + block_len], 1.0)
    coherence[...] = ratio.T
    peak[...] = jnp.max(ratio, axis=0, keepdims=True)


def largest(value, axes):
    total = lax.axis_size(axes)
    if total <= 4:
        others = [turned_about(value, axes, steps) for steps in range(1, total)]
        return functools.reduce(jnp.maximum, others, value)
    for axis in axes[::-1]:
        count = lax.axis_size(axis)
        step = 1
        if count & (count - 1):
            value = lax.pmax(value, axis)
            continue
        while step < count:
            other = lax.ppermute(value, axis, [(i, i ^ step) for i in range(count)])
            value = jnp.maximum(value, other)
            step *= 2
    return value


def on_device(traces, slopes, offsets, live):
    groups = lax.axis_size("rx")
    rows, block_len = traces.shape
    width = slopes.shape[0] // groups
    rest = SPAN + WIN
    cols = block_len + WIN
    place = lax.axis_index("rx").astype(jnp.int32).reshape(1)
    halo = passed_along(traces[:, :rest], ("ta", "af"), -1)
    order = [0] + [d for pair in zip(range(1, groups), range(groups - 1, 0, -1)) for d in pair][: groups - 1]
    order = list(dict.fromkeys(order))
    longer = jnp.concatenate([traces, halo], axis=1)
    moved = {d: near(longer if d == 0 else turned_about(longer, "rx", d)) for d in order}
    calls = [part for part in (order[:1], order[1:3], order[3:]) if part]
    slope_rows = slopes.reshape(groups, 1, width)
    if width % 128:
        slope_rows = jnp.tile(slope_rows, (1, 1, LANES // width))
    gain = live.reshape(groups, 1, rows)
    offset_rows = offsets.reshape(groups, 1, rows)
    partial = []
    for number, part in enumerate(calls):
        final = number == len(calls) - 1
        share = pltpu.VMEM((2 * cols, width), jnp.float32)
        panel = jax.ShapeDtypeStruct((width, block_len), jnp.float32)
        crest = pltpu.VMEM((1, width), jnp.float32)
        tall = 2 * (cols + PACK)
        vmem = pl.BlockSpec(memory_space=pltpu.VMEM)
        result = pl.pallas_call(
            functools.partial(
                stack_kernel,
                away=part,
                groups=groups,
                cols=cols,
                block_len=block_len,
                first=number == 0,
                final=final,
            ),
            in_specs=[pl.BlockSpec(memory_space=pltpu.SMEM)] + [vmem] * (3 + len(part) + len(partial)),
            out_shape=(panel, panel, crest) if final else share,
            scratch_shapes=[
                pltpu.VMEM((2 * cols, width), jnp.float32),
                pltpu.VMEM((tall, rows * (SPAN // PACK)), jnp.bfloat16),
                pltpu.VMEM((rows, LANES), jnp.bfloat16),
                pltpu.VMEM((tall, LANES), jnp.float32),
            ],
            name=f"stack{number}",
        )(
            place,
            slope_rows,
            gain,
            offset_rows,
            *[moved[d] for d in part],
            *partial,
        )
        partial = [] if final else [near(result)]
    stack, coherence, peak = result
    return (stack, coherence, largest(peak, ("ta", "af")).reshape(width))


def solution(mesh):
    placed = (P(("shots", "rx"), ("ta", "af")), P(), P("shots"), P("shots"))
    return jax.shard_map(
        on_device,
        mesh=mesh,
        in_specs=placed,
        out_specs=(
            P(("shots", "rx"), ("ta", "af")),
            P(("shots", "rx"), ("ta", "af")),
            P(("shots", "rx")),
        ),
        check_vma=False,
    )
```

```python
import functools

import jax
import jax.numpy as jnp
from jax import lax
from jax.experimental import pallas as pl
from jax.experimental.pallas import tpu as pltpu
from jax.sharding import PartitionSpec as P

SPAN = 64
WIN = 16
PACK = 16
LANES = 256


def passed_along(value, axis, steps):
    count = lax.axis_size(axis)
    leading, last = (max(0, -steps), min(count, count - steps))
    return lax.ppermute(value, axis, [(source, source + steps) for source in range(leading, last)])


def turned_about(value, axis, steps):
    count = lax.axis_size(axis)
    return lax.ppermute(value, axis, [(i, (i + steps) % count) for i in range(count)])


def near(value):
    return pltpu.with_memory_space_constraint(value, pltpu.VMEM)


def stack_kernel(*refs, away, groups, cols, block_len, first, final):
    count = len(away)
    place, slopes, gain, offsets = refs[:4]
    traces = refs[4 : 4 + count]
    refs = refs[4 + count :]
    if not first:
        before, refs = refs[0], refs[1:]
    if final:
        stack, coherence, peak = refs[:3]
        refs = refs[3:]
    else:
        out, refs = refs[0], refs[1:]
    total, left, right_hits, product = refs
    rows = traces[0].shape[1]
    tall = cols + PACK
    width = total.shape[1]
    reps = LANES // width
    me = place[0]
    slope_row = slopes[me].astype(jnp.float32)
    if slope_row.shape[1] < LANES:
        slope_row = jnp.concatenate([slope_row] * reps, axis=1)
    lag_row = lax.broadcasted_iota(jnp.int32, (1, LANES), 1) // width
    steps = SPAN // PACK
    if first:
        total[...] = jnp.zeros_like(total)
    else:
        total[...] = before[...]
    for index, distance in enumerate(away):
        group = lax.rem(me + (groups - distance), groups)
        live = gain[group].astype(jnp.float32)
        weighted = traces[index][...].astype(jnp.float32) * live
        squares = weighted * weighted
        for step in range(steps):
            at = step * PACK
            here = slice(step * rows, (step + 1) * rows)
            left[0:tall, here] = weighted[at : at + tall].astype(jnp.bfloat16)
            left[tall:, here] = squares[at : at + tall].astype(jnp.bfloat16)
        offset_col = jnp.broadcast_to(offsets[group].astype(jnp.float32), (128, rows)).T[:, 0:1]
        delays = (offset_col * slope_row).astype(jnp.int32) >> 16
        right_hits[...] = (delays - lag_row).astype(jnp.float32).astype(jnp.bfloat16)
        for base in range(0, PACK, reps):
            hits = [
                jnp.where(right_hits[...] == jnp.bfloat16(step * PACK + base), jnp.bfloat16(1), jnp.bfloat16(0))
                for step in range(steps)
            ]
            product[...] = jnp.dot(
                left[...], jnp.concatenate(hits, axis=0), preferred_element_type=jnp.float32
            )
            for rep in range(reps):
                lanes = slice(rep * width, (rep + 1) * width)
                down = base + rep
                total[0:cols] += product[down : down + cols, lanes]
                total[cols:] += product[tall + down : tall + down + cols, lanes]
    if not final:
        out[...] = total[...]
        return
    result = total[...]
    stack[...] = result[:block_len].T
    total[0:cols] = result[:cols] * result[:cols]
    length, reach = cols, 1
    while reach < WIN:
        length = length - reach
        for start in (0, cols):
            total[start : start + length] = (
                total[start : start + length] + total[start + reach : start + reach + length]
            )
        reach *= 2
    ratio = total[0:block_len] / jnp.maximum(total[cols : cols + block_len], 1.0)
    coherence[...] = ratio.T
    peak[...] = jnp.max(ratio, axis=0, keepdims=True)


def largest(value, axes):
    for axis in axes[::-1]:
        count = lax.axis_size(axis)
        step = 1
        if count & (count - 1):
            value = lax.pmax(value, axis)
            continue
        while step < count:
            other = lax.ppermute(value, axis, [(i, i ^ step) for i in range(count)])
            value = jnp.maximum(value, other)
            step *= 2
    return value


def on_device(traces, slopes, offsets, live):
    groups = lax.axis_size("rx")
    rows, block_len = traces.shape
    width = slopes.shape[0] // groups
    rest = SPAN + WIN
    cols = block_len + WIN
    place = lax.axis_index("rx").astype(jnp.int32).reshape(1)
    turned = traces.T
    halo = passed_along(turned[:rest], ("ta", "af"), -1)
    order = [0] + [d for pair in zip(range(1, groups), range(groups - 1, 0, -1)) for d in pair][: groups - 1]
    order = list(dict.fromkeys(order))
    longer = jnp.concatenate([turned, halo], axis=0)
    moved = {d: near(longer if d == 0 else turned_about(longer, "rx", d)) for d in order}
    calls = [part for part in (order[:1], order[1:3], order[3:]) if part]
    slope_rows = slopes.reshape(groups, 1, width)
    if width % 128:
        slope_rows = jnp.tile(slope_rows, (1, 1, LANES // width))
    gain = live.reshape(groups, 1, rows)
    offset_rows = offsets.reshape(groups, 1, rows)
    partial = []
    for number, part in enumerate(calls):
        final = number == len(calls) - 1
        share = pltpu.VMEM((2 * cols, width), jnp.float32)
        panel = jax.ShapeDtypeStruct((width, block_len), jnp.float32)
        crest = pltpu.VMEM((1, width), jnp.float32)
        tall = 2 * (cols + PACK)
        vmem = pl.BlockSpec(memory_space=pltpu.VMEM)
        result = pl.pallas_call(
            functools.partial(
                stack_kernel,
                away=part,
                groups=groups,
                cols=cols,
                block_len=block_len,
                first=number == 0,
                final=final,
            ),
            in_specs=[pl.BlockSpec(memory_space=pltpu.SMEM)] + [vmem] * (3 + len(part) + len(partial)),
            out_shape=(panel, panel, crest) if final else share,
            scratch_shapes=[
                pltpu.VMEM((2 * cols, width), jnp.float32),
                pltpu.VMEM((tall, rows * (SPAN // PACK)), jnp.bfloat16),
                pltpu.VMEM((rows, LANES), jnp.bfloat16),
                pltpu.VMEM((tall, LANES), jnp.float32),
            ],
            name=f"stack{number}",
        )(
            place,
            slope_rows,
            gain,
            offset_rows,
            *[moved[d] for d in part],
            *partial,
        )
        partial = [] if final else [near(result)]
    stack, coherence, peak = result
    return (stack, coherence, largest(peak, ("ta", "af")).reshape(width))


def solution(mesh):
    placed = (P(("shots", "rx"), ("ta", "af")), P(), P("shots"), P("shots"))
    return jax.shard_map(
        on_device,
        mesh=mesh,
        in_specs=placed,
        out_specs=(
            P(("shots", "rx"), ("ta", "af")),
            P(("shots", "rx"), ("ta", "af")),
            P(("shots", "rx")),
        ),
        check_vma=False,
    )
```
